32 devices in a mesh: gx: 4 (over y, x), gy: 2 (over core), gz: 4 (over z).
Axes of the slice: x: 2, y: 2, z: 4, core: 2. Of those that a mesh axis runs over, the one named last changes fastest.
Arguments:
- pair: bfloat16 [128, 1024, 1024], P('gz', 'gy', 'gx'), may hold values from -6 to 6
- pair_mask: int32 [1024, 1024], P('gy', 'gx'), may hold values 0 or 1
- in_gain: float32 [128], replicated, may hold values from 0.5 to 2
- w_left: bfloat16 [128, 128], P(None, 'gz'), may hold values from -0.5 to 0.5
- w_left_gate: bfloat16 [128, 128], P(None, 'gz'), may hold values from -0.5 to 0.5
- w_right: bfloat16 [128, 128], P(None, 'gz'), may hold values from -0.5 to 0.5
- w_right_gate: bfloat16 [128, 128], P(None, 'gz'), may hold values from -0.5 to 0.5
- w_out_gate: bfloat16 [128, 128], P(None, 'gz'), may hold values from -0.5 to 0.5
- out_gain: float32 [128], P('gz'), may hold values from 0.5 to 2
- w_out: bfloat16 [128, 128], P(None, 'gz'), may hold values from -0.5 to 0.5
Outputs:
- update: bfloat16 [128, 1024, 1024], P('gz', 'gy', 'gx')
The draws below stay inside these ranges and needn't reach their ends.
All inputs are finite; a program needn't handle non-finite values. No bound on the sum of `pair_mask` on one device may be relied on, other than what follows from the above.
Results may differ from the reference program's by a relative error of at most 0.0078.
Values may be sent and summed in bfloat16 or wider, within the bound.
A program may use at most 192 MiB of HBM per device.

```python
import math
import jax
import jax.numpy as jnp
from jax import lax

CZ = 128
CH = 128
N = 1024


def set_ends(values, own_key, smallest, high):
    longest = values.shape.index(max(values.shape))
    spots = []
    for shift in (0, 1):
        where = [jax.random.randint(jax.random.fold_in(own_key, axis), (), 0, length) for axis, length in enumerate(values.shape)]
        where[longest] = (where[longest] + shift) % values.shape[longest]
        spots.append(tuple(where))
    return values.at[spots[0]].set(smallest).at[spots[1]].set(high)


def block_levels(own_key, shape, shards, least, top_value):
    level, own = 1.0, jax.random.fold_in(own_key, 6)
    for dim, shards_of in shards:
        steps = jnp.exp(jax.random.uniform(jax.random.fold_in(own, dim), (shards_of,), jnp.float32, least / len(shards), top_value / len(shards)))
        level = level * jnp.repeat(steps, shape[dim] // shards_of).reshape([-1 if axis == dim else 1 for axis in range(len(shape))])
    return level


def normal_values(key, dims, deviation, bound, cuts=(), held_as=jnp.bfloat16):
    entries = jax.random.normal(key, dims, jnp.float32) * deviation
    if len(cuts) > 0:
        entries = block_levels(key, dims, cuts, -0.22, 0.18) * entries
    return jnp.clip(entries, min=-bound, max=bound).astype(held_as)


def setup_inputs(seed: int = 0) -> dict:
    arg_keys = jax.random.split(jax.random.key(seed), 11)
    pair = normal_values(arg_keys[0], (CZ, N, N), 1.0, 6.0, ((0, 4), (1, 2), (2, 4)))
    pair_mask = set_ends((jax.random.randint(arg_keys[1], (N, N), 0, 8) < 7).astype(jnp.int32), jax.random.fold_in(arg_keys[1], 1), 0, 1)
    in_gain = jnp.clip(jnp.exp(jax.random.uniform(arg_keys[2], (CZ,), jnp.float32, math.log(0.5), math.log(2.0))), 0.5, 2.0)
    w_left = normal_values(arg_keys[3], (CZ, CH), CZ ** -0.5, 0.5, ((1, 4),))
    w_left_gate = normal_values(arg_keys[4], (CZ, CH), CZ ** -0.5, 0.5, ((1, 4),))
    w_right = normal_values(arg_keys[5], (CZ, CH), CZ ** -0.5, 0.5, ((1, 4),))
    w_right_gate = normal_values(arg_keys[6], (CZ, CH), CZ ** -0.5, 0.5, ((1, 4),))
    w_out_gate = normal_values(arg_keys[7], (CZ, CZ), CZ ** -0.5, 0.5, ((1, 4),))
    out_gain = jnp.clip(jnp.exp(math.log(2.0) - 1.3862944 * jax.random.uniform(arg_keys[8], (CH,), jnp.float32) ** block_levels(arg_keys[8], (CH,), ((0, 4),), -0.2, 0.2)), 0.5, 2.0)
    w_out = normal_values(arg_keys[9], (CH, CZ), CH ** -0.5, 0.5, ((1, 4),))
    return {"pair": pair, "pair_mask": pair_mask, "in_gain": in_gain, "w_left": w_left, "w_left_gate": w_left_gate, "w_right": w_right, "w_right_gate": w_right_gate, "w_out_gate": w_out_gate, "out_gain": out_gain, "w_out": w_out}


epsilon = 1e-05

def layer_norm(values, gain):
    average = lax.optimization_barrier(jnp.mean(values, axis=0))
    centered = values - average
    spread = lax.optimization_barrier(jnp.mean(jnp.square(centered), axis=0))
    return centered * lax.rsqrt(spread + epsilon) * gain[:, None, None]

def reference(pair, pair_mask, in_gain, w_left, w_left_gate, w_right, w_right_gate, w_out_gate, out_gain, w_out):
    normed = layer_norm(pair.astype(jnp.float32), in_gain).astype(jnp.bfloat16)
    normed_f = normed.astype(jnp.float32)
    mask_float = pair_mask.astype(jnp.float32)[None]

    def project(weight):
        return jnp.einsum('cik,ch->hik', normed_f, weight.astype(jnp.float32))
    left_rows = (mask_float * jax.nn.sigmoid(project(w_left_gate)) * project(w_left)).astype(jnp.bfloat16)
    right_rows = (mask_float * jax.nn.sigmoid(project(w_right_gate)) * project(w_right)).astype(jnp.bfloat16)

    def channel_product(operands):
        return jnp.dot(operands[0], operands[1].T, preferred_element_type=jnp.float32)
    mixed_sum = lax.map(channel_product, (left_rows, right_rows))
    normed_mix = layer_norm(mixed_sum, out_gain).astype(jnp.bfloat16)
    out_gate = jax.nn.sigmoid(jnp.einsum('cij,cd->dij', normed_f, w_out_gate.astype(jnp.float32)))
    projected = jnp.einsum('hij,hd->dij', normed_mix.astype(jnp.float32), w_out.astype(jnp.float32))
    return (out_gate * projected).astype(jnp.bfloat16)
```

```python
import functools
import itertools
import math

import jax
import jax.numpy as jnp
from jax import lax
from jax.experimental import pallas as pl
from jax.experimental.pallas import tpu as pltpu
from jax.sharding import PartitionSpec as P

epsilon = 1e-05
MESH = pl.DeviceIdType.MESH


def exchange_kernel(axes, sizes, take, put, x_ref, o_ref, send_sem, recv_sem, local_sem):
    me = tuple(lax.axis_index(axis) for axis in axes)
    offsets = [o for o in itertools.product(*(range(n) for n in sizes)) if any(o)]

    def peer_of(offset):
        return tuple(lax.rem(m + o, n) for m, o, n in zip(me, offset, sizes))

    barrier = pltpu.get_barrier_semaphore()
    for offset in offsets:
        pl.semaphore_signal(
            barrier, inc=1, device_id=dict(zip(axes, peer_of(offset))), device_id_type=MESH
        )
    pl.semaphore_wait(barrier, len(offsets))
    copies = []
    for index, offset in enumerate(offsets):
        peer = peer_of(offset)
        copy = pltpu.make_async_remote_copy(
            src_ref=take(x_ref, peer),
            dst_ref=put(o_ref, me),
            send_sem=send_sem.at[index],
            recv_sem=recv_sem.at[index],
            device_id=dict(zip(axes, peer)),
            device_id_type=MESH,
        )
        copy.start()
        copies.append(copy)
    own = pltpu.make_async_copy(take(x_ref, me), put(o_ref, me), local_sem)
    own.start()
    own.wait()
    for copy in copies:
        copy.wait()


def exchange(x, axes, shape, take, put, collective_id):
    sizes = tuple(lax.axis_size(axis) for axis in axes)
    count = math.prod(sizes) - 1
    moved = x.size * x.dtype.itemsize
    return pl.pallas_call(
        functools.partial(exchange_kernel, axes, sizes, take, put),
        out_shape=jax.ShapeDtypeStruct(shape, x.dtype),
        in_specs=[pl.BlockSpec(memory_space=pl.ANY)],
        out_specs=pl.BlockSpec(memory_space=pl.ANY),
        scratch_shapes=[
            pltpu.SemaphoreType.DMA((count,)),
            pltpu.SemaphoreType.DMA((count,)),
            pltpu.SemaphoreType.DMA,
        ],
        compiler_params=pltpu.CompilerParams(collective_id=collective_id, has_side_effects=True),
        cost_estimate=pl.CostEstimate(flops=0, bytes_accessed=20 * moved, transcendentals=0),
    )(x)


def normalize(values, gain):
    average = jnp.mean(values, axis=0, keepdims=True)
    centered = values - average
    spread = jnp.mean(jnp.square(centered), axis=0, keepdims=True)
    return (centered * lax.rsqrt(spread + epsilon) * gain).astype(jnp.bfloat16)


def project_kernel(x_ref, mask_ref, gain_ref, weight_ref, left_ref, right_ref, gate_ref):
    rows = x_ref.shape[0]
    h = left_ref.shape[1]
    gain = gain_ref[...]

    def body(row, carry):
        normed = normalize(x_ref[row].astype(jnp.float32), gain)
        mask = mask_ref[pl.ds(row, 1), :]

        def part(index):
            return jnp.dot(
                weight_ref[index * h : (index + 1) * h, :],
                normed,
                preferred_element_type=jnp.float32,
            )

        left_ref[row] = (mask * jax.nn.sigmoid(part(1)) * part(0)).astype(jnp.bfloat16)
        right_ref[row] = (mask * jax.nn.sigmoid(part(3)) * part(2)).astype(jnp.bfloat16)
        gate_ref[row] = jax.nn.sigmoid(part(4)).astype(jnp.bfloat16)
        return carry

    lax.fori_loop(0, rows, body, 0)


def finish_kernel(mix_ref, gate_ref, gain_ref, weight_ref, out_ref):
    gain = gain_ref[...]

    def body(row, carry):
        normed = normalize(mix_ref[row].astype(jnp.float32), gain)
        projected = jnp.dot(weight_ref[...], normed, preferred_element_type=jnp.float32)
        out_ref[row] = (gate_ref[row].astype(jnp.float32) * projected).astype(jnp.bfloat16)
        return carry

    lax.fori_loop(0, mix_ref.shape[0], body, 0)


def local(
    pair,
    pair_mask,
    in_gain,
    w_left,
    w_left_gate,
    w_right,
    w_right_gate,
    w_out_gate,
    out_gain,
    w_out,
):
    nx, nz = lax.axis_size("gx"), lax.axis_size("gz")
    channels, i_rows, k_columns = pair.shape
    c_all = channels * nz
    rows = i_rows // nz
    h_all = w_left.shape[1] * nz
    h_own = h_all // (nx * nz)
    stacked = jnp.stack([w_left, w_left_gate, w_right, w_right_gate, w_out_gate, w_out])
    weights = jnp.swapaxes(lax.all_gather(stacked, "gz", axis=2, tiled=True), 1, 2)
    gain_mix = lax.all_gather(out_gain, "gz", axis=0, tiled=True)
    mask_rows = lax.dynamic_slice_in_dim(
        pair_mask, lax.axis_index("gz") * rows, rows, axis=0
    ).astype(jnp.float32)

    gathered = exchange(
        jnp.swapaxes(pair, 0, 1),
        ("gz",),
        (rows, c_all, k_columns),
        lambda ref, dev: ref.at[pl.ds(dev[0] * rows, rows)],
        lambda ref, dev: ref.at[:, pl.ds(pl.multiple_of(dev[0] * channels, channels), channels)],
        0,
    )

    block = 8
    row_spec = pl.BlockSpec((block, c_all, k_columns), lambda i: (i, 0, 0))
    h_spec = pl.BlockSpec((block, h_all, k_columns), lambda i: (i, 0, 0))
    whole = lambda *shape: pl.BlockSpec(shape, lambda i: (0,) * len(shape))
    h_shape = jax.ShapeDtypeStruct((rows, h_all, k_columns), jnp.bfloat16)
    left_rows, right_rows, out_gate = pl.pallas_call(
        project_kernel,
        grid=(rows // block,),
        out_shape=(h_shape, h_shape, h_shape),
        in_specs=[
            row_spec,
            pl.BlockSpec((block, k_columns), lambda i: (i, 0)),
            whole(c_all, 1),
            whole(5 * h_all, c_all),
        ],
        out_specs=(h_spec, h_spec, h_spec),
    )(gathered, mask_rows, in_gain[:, None], weights[:5].reshape(5 * h_all, c_all))

    def block_of(ref, dev):
        return ref.at[
            :,
            pl.ds(pl.multiple_of(dev[1] * rows, rows), rows),
            pl.ds(pl.multiple_of(dev[0] * k_columns, k_columns), k_columns),
        ]

    def heads_of(ref, dev):
        return ref.at[pl.ds((dev[0] * nz + dev[1]) * h_own, h_own)]

    group_shape = (h_own, i_rows, k_columns * nx)
    right_group = exchange(
        jnp.swapaxes(right_rows, 0, 1), ("gx", "gz"), group_shape, heads_of, block_of, 1
    )
    right_all = lax.all_gather(right_group, "gy", axis=1, tiled=True)
    left_group = exchange(
        jnp.swapaxes(left_rows, 0, 1), ("gx", "gz"), group_shape, heads_of, block_of, 2
    )
    mixed = lax.dot_general(
        left_group,
        right_all,
        (((2,), (2,)), ((0,), (0,))),
        preferred_element_type=jnp.float32,
    ).astype(jnp.bfloat16)
    mix = exchange(
        mixed, ("gx", "gz"), (h_all, rows, k_columns), block_of, heads_of, 3
    )
    update = pl.pallas_call(
        finish_kernel,
        grid=(rows // block,),
        out_shape=h_shape,
        in_specs=[h_spec, h_spec, whole(h_all, 1), whole(h_all, h_all)],
        out_specs=h_spec,
    )(jnp.swapaxes(mix, 0, 1), out_gate, gain_mix[:, None], weights[5])
    result = exchange(
        update,
        ("gz",),
        (i_rows, channels, k_columns),
        lambda ref, dev: ref.at[:, pl.ds(pl.multiple_of(dev[0] * channels, channels), channels)],
        lambda ref, dev: ref.at[pl.ds(dev[0] * rows, rows)],
        4,
    )
    return jnp.swapaxes(result, 0, 1)


def solution(mesh):
    placed = (
        P("gz", "gy", "gx"),
        P("gy", "gx"),
        P(),
        P(None, "gz"),
        P(None, "gz"),
        P(None, "gz"),
        P(None, "gz"),
        P(None, "gz"),
        P("gz"),
        P(None, "gz"),
    )
    return jax.shard_map(
        local, mesh=mesh, in_specs=placed, out_specs=P("gz", "gy", "gx"), check_vma=False
    )
```
